32 devices in a mesh: dp: 4 (over y, z), ep: 8 (over x, core).
Axes of the slice: x: 4, y: 2, z: 2, core: 2. Of those that a mesh axis runs over, the one named last changes fastest.
The devices are a block of a 4x4x8 slice.
Arguments:
- hidden: bfloat16 [4096, 2304], P(('dp', 'ep')), parts along dimension 0
- expert_ids: int32 [4096, 2], P(('dp', 'ep')), parts along dimension 0
- norm_gain: bfloat16 [2304], replicated
- w_router: bfloat16 [2304, 8], replicated
- w_gate: bfloat16 [8, 2304, 5760], P('ep')
- w_up: bfloat16 [8, 2304, 5760], P('ep')
- w_down: bfloat16 [8, 5760, 2304], P('ep')
Outputs:
- output: bfloat16 [4096, 2304], P(('dp', 'ep')), parts along dimension 0
There are 4 independent parts. The reference program is written for one: setup_inputs(seed, part) draws one part's arguments, and reference() takes and returns one part's arrays. A program takes and returns all parts, laid end to end along the dimension named above; an argument that names none is the same for every part.
All inputs are finite; a program needn't handle non-finite values.
Results may differ from the reference program's by a relative error of at most 0.001.
Values are sent between devices in bfloat16 or wider.
A program may use at most 768 MiB of HBM per device.

```python
import jax
import jax.numpy as jnp
from jax import lax

D = 2304
FF = 5760
EXPERTS = 8
TOK = 128
GROUP = 8
NORM_EPS = 1e-5
TOKENS = TOK * GROUP
CAPACITY = (5 * TOK + 2 * EXPERTS - 1) // (2 * EXPERTS)


def draw_expert_ids(key):
    k_hot, k_ticket, k_cover, k_offset = jax.random.split(key, 4)
    hot_expert = jax.random.randint(k_hot, (GROUP, 1), 0, EXPERTS)
    ticket = jax.random.randint(k_ticket, (GROUP, TOK), 0, EXPERTS + 3)
    first_pick = jnp.where(ticket < EXPERTS, ticket, hot_expert)
    token_pos = jnp.arange(TOK)[None, :]
    cover_shift = jax.random.randint(k_cover, (GROUP, 1), 0, EXPERTS)
    first_pick = jnp.where(token_pos < EXPERTS, (token_pos + cover_shift) % EXPERTS, first_pick)
    offset = jax.random.randint(k_offset, (GROUP, TOK), 1, EXPERTS)
    second_pick = (first_pick + offset) % EXPERTS
    return jnp.stack([first_pick, second_pick], axis=-1).reshape(TOKENS, 2).astype(jnp.int32)


def setup_inputs(seed: int = 0, part: int = 0) -> dict:
    key = jax.random.key(seed)
    k_hidden, k_ids, k_gain, k_router, k_gate, k_up, k_down = jax.random.split(key, 7)
    k_hidden = jax.random.fold_in(k_hidden, part)
    k_ids = jax.random.fold_in(k_ids, part)
    hidden = jax.random.normal(k_hidden, (TOKENS, D), jnp.float32).astype(jnp.bfloat16)
    expert_ids = draw_expert_ids(k_ids)
    norm_gain = (1.0 + 0.3 * jax.random.normal(k_gain, (D,), jnp.float32)).astype(jnp.bfloat16)
    w_router = (2.0 * D ** -0.5 * jax.random.normal(k_router, (D, EXPERTS), jnp.float32)).astype(jnp.bfloat16)
    w_gate = (D ** -0.5 * jax.random.normal(k_gate, (EXPERTS, D, FF), jnp.float32)).astype(jnp.bfloat16)
    w_up = (D ** -0.5 * jax.random.normal(k_up, (EXPERTS, D, FF), jnp.float32)).astype(jnp.bfloat16)
    w_down = (2.0 * FF ** -0.5 * jax.random.normal(k_down, (EXPERTS, FF, D), jnp.float32)).astype(jnp.bfloat16)
    return {"hidden": hidden, "expert_ids": expert_ids, "norm_gain": norm_gain, "w_router": w_router, "w_gate": w_gate, "w_up": w_up, "w_down": w_down}


def rms_norm(hidden, norm_gain):
    hidden_f32 = hidden.astype(jnp.float32)
    mean_sq = jnp.mean(hidden_f32 * hidden_f32, axis=-1, keepdims=True)
    return (hidden_f32 * lax.rsqrt(mean_sq + NORM_EPS) * norm_gain.astype(jnp.float32)).astype(jnp.bfloat16)


def slot_positions(shard_ids):
    slot_order = jnp.concatenate([shard_ids[:, 0], shard_ids[:, 1]])
    hit_table = (slot_order[:, None] == jnp.arange(EXPERTS)[None, :]).astype(jnp.int32)
    seen_before = jnp.cumsum(hit_table, axis=0) - hit_table
    slot_rank = jnp.sum(seen_before * hit_table, axis=1)
    return slot_rank.reshape(2, TOK).T


def expert_ffn(operands):
    rows, gate_w, up_w, down_w = operands
    gate_proj = jnp.dot(rows, gate_w, preferred_element_type=jnp.float32)
    up_proj = jnp.dot(rows, up_w, preferred_element_type=jnp.float32)
    hidden_act = (jax.nn.silu(gate_proj) * up_proj).astype(jnp.bfloat16)
    return jnp.dot(hidden_act, down_w, preferred_element_type=jnp.float32).astype(jnp.bfloat16)


def reference(hidden, expert_ids, norm_gain, w_router, w_gate, w_up, w_down):
    normed = rms_norm(hidden, norm_gain)
    logits = jnp.dot(normed, w_router, preferred_element_type=jnp.float32)
    picked = jnp.take_along_axis(logits, expert_ids, axis=1)
    gate_probs = jax.nn.softmax(picked, axis=-1)
    positions = jax.vmap(slot_positions)(expert_ids.reshape(GROUP, TOK, 2)).reshape(TOKENS, 2)
    source = (jnp.arange(TOKENS) // TOK)[:, None]
    kept = positions < CAPACITY
    buffer_row = jnp.where(kept, source * CAPACITY + positions, GROUP * CAPACITY)
    rows_in = jnp.broadcast_to(normed[:, None, :], (TOKENS, 2, D))
    buffers = jnp.zeros((EXPERTS, GROUP * CAPACITY, D), jnp.bfloat16)
    buffers = buffers.at[expert_ids, buffer_row].set(rows_in, mode="drop")
    expert_out = lax.map(expert_ffn, (buffers, w_gate, w_up, w_down))
    fetched = expert_out[expert_ids, jnp.minimum(buffer_row, GROUP * CAPACITY - 1)]
    fetched = jnp.where(kept[:, :, None], fetched.astype(jnp.float32), 0.0)
    mixed_sum = jnp.sum(gate_probs[:, :, None] * fetched, axis=1)
    return (hidden.astype(jnp.float32) + mixed_sum).astype(jnp.bfloat16)
```

```python
import functools

import jax
import jax.numpy as jnp
from jax import lax
from jax.experimental import pallas as pl
from jax.experimental.pallas import tpu as pltpu
from jax.sharding import PartitionSpec as P

NORM_EPS = 1e-5
CHIPS = 4
BLOCKS = 8
FCOLS = 640
NCOLS = 256
K_CHUNKS = (256, 512, 512, 512, 512)
WD_SLOTS = 3


def block_pairs():
    return [(d, s) for d in (2, 1, 3, 0) for s in (0, 1) if (d, s) != (0, 0)]


def moe_kernel(cap, x_hbm, ids_hbm, gain_hbm, router_hbm, wg_hbm, wu_hbm, wd_hbm, out_hbm,
               x_v, ids_v, gain_v, router_v, u_v, w_ring, wd_ring, acc, h_v, u2_v, o_stage, back, out_v, *rest):
    nk = len(K_CHUNKS)
    stage = rest[:nk]
    recv = rest[nk:2 * nk]
    in_sem, w_sem, wd_sem, ds_sem, dr_sem, os_sem, or_sem, out_sem = rest[2 * nk:]
    rows, width = x_v.shape
    ff = h_v.shape[1]
    slots = BLOCKS * cap
    n_f = ff // FCOLS
    n_n = width // NCOLS
    k_off = [sum(K_CHUNKS[:i]) for i in range(nk)]

    me = lax.axis_index("ep")
    chip = me // 2
    core = me % 2

    def peer(d, s):
        return {"ep": lax.rem(chip + d, CHIPS) * 2 + lax.rem(core + s, 2)}

    in_copies = [pltpu.make_async_copy(a, b, in_sem.at[i]) for i, (a, b) in enumerate(
        ((x_hbm, x_v), (ids_hbm, ids_v), (gain_hbm, gain_v), (router_hbm, router_v)))]
    for cp in in_copies:
        cp.start()

    def w_copies(kc, f):
        slot = (kc % 2) * n_f + f
        rows_k = pl.ds(k_off[kc], K_CHUNKS[kc])
        cols = pl.ds(pl.multiple_of(f * FCOLS, 128), FCOLS)
        dst = w_ring.at[slot, pl.ds(0, K_CHUNKS[kc])]
        return (pltpu.make_async_copy(wg_hbm.at[0, rows_k, cols], dst.at[:, pl.ds(0, FCOLS)], w_sem.at[slot, 0]),
                pltpu.make_async_copy(wu_hbm.at[0, rows_k, cols], dst.at[:, pl.ds(FCOLS, FCOLS)], w_sem.at[slot, 1]))

    def wd_copy(n, slot):
        cols = pl.ds(pl.multiple_of(n * NCOLS, 128), NCOLS)
        return pltpu.make_async_copy(wd_hbm.at[0, :, cols], wd_ring.at[slot], wd_sem.at[slot])

    barrier = pltpu.get_barrier_semaphore()
    for d, s in block_pairs():
        pl.semaphore_signal(barrier, inc=1, device_id=peer(d, s))

    for kc in range(2):
        @pl.loop(0, n_f)
        def _(f):
            for cp in w_copies(kc, f):
                cp.start()

    for cp in in_copies:
        cp.wait()

    xf = x_v[...].astype(jnp.float32)
    mean_sq = jnp.sum(xf * xf, axis=-1, keepdims=True) * (1.0 / width)
    u = (xf * lax.rsqrt(mean_sq + NORM_EPS) * gain_v[...].astype(jnp.float32)).astype(jnp.bfloat16)
    u_v[...] = u

    ids0 = ids_v[:, 0:1]
    ids1 = ids_v[:, 1:2]
    lane = lax.broadcasted_iota(jnp.int32, (rows, 128), 1)
    hit0 = jnp.where(lane == ids0, 1.0, 0.0).astype(jnp.float32)
    hit1 = jnp.where(lane == ids1 + BLOCKS, 1.0, 0.0).astype(jnp.float32)
    before = jnp.where(lax.broadcasted_iota(jnp.int32, (rows, rows), 0) > lax.broadcasted_iota(jnp.int32, (rows, rows), 1),
                       1.0, 0.0).astype(jnp.bfloat16)
    seen = jnp.dot(before, (hit0 + hit1).astype(jnp.bfloat16), preferred_element_type=jnp.float32)
    total0 = jnp.sum(hit0, axis=0, keepdims=True)
    pos0 = jnp.sum(seen * hit0, axis=1, keepdims=True)
    pos1 = jnp.sum(seen * hit1 + jnp.where(lane == ids1, total0, 0.0), axis=1, keepdims=True)

    def slot_of(ids, pos):
        block = ((((ids >> 1) - chip) & (CHIPS - 1)) << 1) | ((ids & 1) ^ core)
        return jnp.where(pos < cap, (block * cap).astype(jnp.float32) + pos, -1.0)

    slot0 = slot_of(ids0, pos0)
    slot1 = slot_of(ids1, pos1)
    slot_iota = lax.broadcasted_iota(jnp.int32, (rows, 384), 1).astype(jnp.float32)
    take0 = jnp.where(slot_iota == slot0, 1.0, 0.0)
    take1 = jnp.where(slot_iota == slot1, 1.0, 0.0)
    pick = jnp.transpose(take0 + take1)[:slots].astype(jnp.bfloat16)

    def dispatch(kc, wait_barrier):
        cols = pl.ds(k_off[kc], K_CHUNKS[kc])
        part = jnp.dot(pick, u_v[:, cols], preferred_element_type=jnp.float32).astype(jnp.bfloat16)
        stage[kc][pl.ds(0, slots), :] = part
        recv[kc][pl.ds(0, cap), :] = part[:cap]
        if wait_barrier:
            pl.semaphore_wait(barrier, BLOCKS - 1)
        for d, s in block_pairs():
            send_copy(kc, d, s).start()

    def send_copy(kc, d, s):
        b = d * 2 + s
        rb = ((CHIPS - d) % CHIPS) * 2 + s
        return pltpu.make_async_remote_copy(
            src_ref=stage[kc].at[pl.ds(b * cap, cap)], dst_ref=recv[kc].at[pl.ds(rb * cap, cap)],
            send_sem=ds_sem.at[kc, b], recv_sem=dr_sem.at[kc, rb], device_id=peer(d, s))

    for kc in range(nk):
        dispatch(kc, kc == 0)

    logits = jnp.dot(u, router_v[...], preferred_element_type=jnp.float32)
    lane8 = lax.broadcasted_iota(jnp.int32, logits.shape, 1)
    pick0 = jnp.sum(jnp.where(lane8 == ids0, logits, 0.0), axis=1, keepdims=True)
    pick1 = jnp.sum(jnp.where(lane8 == ids1, logits, 0.0), axis=1, keepdims=True)
    top = jnp.maximum(pick0, pick1)
    e0 = jnp.exp(pick0 - top)
    e1 = jnp.exp(pick1 - top)
    gate0 = e0 / (e0 + e1)
    gate1 = e1 / (e0 + e1)
    fetch = jnp.concatenate([take0[:, :slots], take1[:, :slots]], axis=0).astype(jnp.bfloat16)

    for kc in range(nk):
        size = K_CHUNKS[kc]
        for d, s in block_pairs():
            send_copy(kc, d, s).wait_recv()
        u2_v[:, pl.ds(0, size)] = recv[kc][pl.ds(0, slots), :]

        @pl.loop(0, n_f)
        def _(f):
            for cp in w_copies(kc, f):
                cp.wait()
            slot = (kc % 2) * n_f + f
            prod = jnp.dot(u2_v[:, pl.ds(0, size)], w_ring[slot, pl.ds(0, size)], preferred_element_type=jnp.float32)
            if kc == 0:
                acc[f] = prod
            elif kc < nk - 1:
                acc[f] = acc[f] + prod
            else:
                g = acc[f, :, pl.ds(0, FCOLS)] + prod[:, :FCOLS]
                v = acc[f, :, pl.ds(FCOLS, FCOLS)] + prod[:, FCOLS:]
                h_v[:, pl.ds(pl.multiple_of(f * FCOLS, 128), FCOLS)] = (jax.nn.silu(g) * v).astype(jnp.bfloat16)
            if kc + 2 < nk:
                for cp in w_copies(kc + 2, f):
                    cp.start()

        if kc == nk - 3:
            for n in range(WD_SLOTS):
                wd_copy(n, n).start()

    def back_copy(n, r, s):
        b = r * 2 + s
        rb = ((CHIPS - r) % CHIPS) * 2 + s
        return pltpu.make_async_remote_copy(
            src_ref=o_stage.at[n, pl.ds(b * cap, cap)], dst_ref=back.at[n, pl.ds(rb * cap, cap)],
            send_sem=os_sem.at[n, b], recv_sem=or_sem.at[n, rb], device_id=peer(r, s))

    @pl.loop(0, n_n)
    def _(n):
        slot = lax.rem(n, WD_SLOTS)
        wd_copy(n, slot).wait()
        o = jnp.dot(h_v[...], wd_ring[slot], preferred_element_type=jnp.float32).astype(jnp.bfloat16)
        o_stage[n, pl.ds(0, slots)] = o
        back[n, pl.ds(0, cap)] = o[:cap]
        for r, s in block_pairs():
            back_copy(n, r, s).start()

        @pl.when(n + WD_SLOTS < n_n)
        def _():
            wd_copy(n + WD_SLOTS, slot).start()

    def out_copy(n):
        cols = pl.ds(pl.multiple_of(n * NCOLS, 128), NCOLS)
        return pltpu.make_async_copy(out_v.at[:, cols], out_hbm.at[:, cols], out_sem.at[n])

    @pl.loop(0, n_n)
    def _(n):
        for r, s in block_pairs():
            back_copy(n, r, s).wait_recv()
        got = jnp.dot(fetch, back[n, pl.ds(0, slots)], preferred_element_type=jnp.float32)
        cols = pl.ds(pl.multiple_of(n * NCOLS, 128), NCOLS)
        y = gate0 * got[:rows] + gate1 * got[rows:]
        out_v[:, cols] = (x_v[:, cols].astype(jnp.float32) + y).astype(jnp.bfloat16)
        out_copy(n).start()

    for kc in range(nk):
        for d, s in block_pairs():
            send_copy(kc, d, s).wait_send()

    @pl.loop(0, n_n)
    def _(n):
        for r, s in block_pairs():
            back_copy(n, r, s).wait_send()
        out_copy(n).wait()


def solution(mesh):
    token_spec = P(("dp", "ep"), None)
    expert_spec = P("ep", None, None)

    def local_block(hidden, expert_ids, norm_gain, w_router, w_gate, w_up, w_down):
        rows, width = hidden.shape
        ff = w_gate.shape[2]
        experts = w_router.shape[1]
        cap = (5 * rows + 2 * experts - 1) // (2 * experts)
        slots = BLOCKS * cap
        padded = slots + 8
        n_f = ff // FCOLS
        n_n = width // NCOLS
        nk = len(K_CHUNKS)
        bf16, f32 = jnp.bfloat16, jnp.float32
        dma = pltpu.SemaphoreType.DMA
        hbm = pl.BlockSpec(memory_space=pl.ANY)
        return pl.pallas_call(
            functools.partial(moe_kernel, cap),
            out_shape=jax.ShapeDtypeStruct((rows, width), bf16),
            in_specs=[hbm] * 7,
            out_specs=hbm,
            scratch_shapes=[
                pltpu.VMEM((rows, width), bf16),
                pltpu.VMEM(expert_ids.shape, jnp.int32),
                pltpu.VMEM((1, width), bf16),
                pltpu.VMEM(w_router.shape, bf16),
                pltpu.VMEM((rows, width), bf16),
                pltpu.VMEM((2 * n_f, max(K_CHUNKS), 2 * FCOLS), bf16),
                pltpu.VMEM((WD_SLOTS, ff, NCOLS), bf16),
                pltpu.VMEM((n_f, slots, 2 * FCOLS), f32),
                pltpu.VMEM((slots, ff), bf16),
                pltpu.VMEM((slots, max(K_CHUNKS)), bf16),
                pltpu.VMEM((n_n, padded, NCOLS), bf16),
                pltpu.VMEM((n_n, padded, NCOLS), bf16),
                pltpu.VMEM((rows, width), bf16),
                *[pltpu.VMEM((padded, k), bf16) for k in K_CHUNKS],
                *[pltpu.VMEM((padded, k), bf16) for k in K_CHUNKS],
                dma((4,)),
                dma((2 * n_f, 2)),
                dma((WD_SLOTS,)),
                dma((nk, BLOCKS)),
                dma((nk, BLOCKS)),
                dma((n_n, BLOCKS)),
                dma((n_n, BLOCKS)),
                dma((n_n,)),
            ],
            compiler_params=pltpu.CompilerParams(collective_id=0, has_side_effects=True, vmem_limit_bytes=67043328),
        )(hidden, expert_ids, norm_gain.reshape(1, width), w_router, w_gate, w_up, w_down)

    return jax.shard_map(local_block, mesh=mesh,
                         in_specs=(token_spec, token_spec, P(None), P(None, None), expert_spec, expert_spec, expert_spec),
                         out_specs=token_spec, check_vma=False)
```

```python
import functools

import jax
import jax.numpy as jnp
from jax import lax
from jax.experimental import pallas as pl
from jax.experimental.pallas import tpu as pltpu
from jax.sharding import PartitionSpec as P

NORM_EPS = 1e-5
CHIPS = 4
BLOCKS = 8
FCOLS = 1920
NCOLS = 256
K_CHUNKS = (256, 512, 512, 512, 512)
WD_SLOTS = 3


def block_pairs():
    return [(d, s) for d in (2, 1, 3, 0) for s in (0, 1) if (d, s) != (0, 0)]


def moe_kernel(cap, x_hbm, ids_hbm, gain_hbm, router_hbm, wg_hbm, wu_hbm, wd_hbm, out_ref,
               x_v, ids_v, gain_v, router_v, u_v, w_ring, wd_ring, acc, h_v, u2_v, o_stage, back, *rest):
    nk = len(K_CHUNKS)
    stage = rest[:nk]
    recv = rest[nk:2 * nk]
    in_sem, w_sem, wd_sem, ds_sem, dr_sem, os_sem, or_sem = rest[2 * nk:]
    rows, width = x_v.shape
    ff = h_v.shape[1]
    slots = BLOCKS * cap
    n_f = ff // FCOLS
    n_n = width // NCOLS
    k_off = [sum(K_CHUNKS[:i]) for i in range(nk)]

    me = lax.axis_index("ep")
    chip = me // 2
    core = me % 2

    def peer(d, s):
        return {"ep": lax.rem(chip + d, CHIPS) * 2 + lax.rem(core + s, 2)}

    in_copies = [pltpu.make_async_copy(a, b, in_sem.at[i]) for i, (a, b) in enumerate(
        ((x_hbm, x_v), (ids_hbm, ids_v), (gain_hbm, gain_v), (router_hbm, router_v)))]
    for cp in in_copies:
        cp.start()

    remote = pl.ds(cap, slots - cap)

    def wait_bytes(ref, sem):
        pltpu.make_async_copy(ref, ref, sem).wait()

    def w_copies(kc, f):
        slot = (kc % 2) * n_f + f
        rows_k = pl.ds(k_off[kc], K_CHUNKS[kc])
        cols = pl.ds(pl.multiple_of(f * FCOLS, 128), FCOLS)
        dst = w_ring.at[slot, pl.ds(0, K_CHUNKS[kc])]
        return (pltpu.make_async_copy(wg_hbm.at[0, rows_k, cols], dst.at[:, pl.ds(0, FCOLS)], w_sem.at[slot]),
                pltpu.make_async_copy(wu_hbm.at[0, rows_k, cols], dst.at[:, pl.ds(FCOLS, FCOLS)], w_sem.at[slot]))

    def wd_copy(n, slot):
        cols = pl.ds(pl.multiple_of(n * NCOLS, 128), NCOLS)
        return pltpu.make_async_copy(wd_hbm.at[0, :, cols], wd_ring.at[slot], wd_sem.at[slot])

    barrier = pltpu.get_barrier_semaphore()
    for d, s in block_pairs():
        pl.semaphore_signal(barrier, inc=1, device_id=peer(d, s))

    for kc in range(2):
        @pl.loop(0, n_f)
        def _(f):
            for cp in w_copies(kc, f):
                cp.start()

    with jax.named_scope('in_wait'):
        for cp in in_copies:
            cp.wait()

    xf = x_v[...].astype(jnp.float32)
    mean_sq = jnp.sum(xf * xf, axis=-1, keepdims=True) * (1.0 / width)
    u = (xf * lax.rsqrt(mean_sq + NORM_EPS) * gain_v[...].reshape(1, width).astype(jnp.float32)).astype(jnp.bfloat16)
    u_v[...] = u

    ids_t = jnp.transpose(jnp.broadcast_to(ids_v[...].astype(jnp.float32)[:, None, :], (2, 8, rows)).reshape(16, rows))
    ids0 = ids_t[:, 0:1].astype(jnp.int32)
    ids1 = ids_t[:, 8:9].astype(jnp.int32)
    lane = lax.broadcasted_iota(jnp.int32, (rows, 128), 1)
    hit0 = jnp.where(lane == ids0, 1.0, 0.0).astype(jnp.float32)
    hit1 = jnp.where(lane == ids1 + BLOCKS, 1.0, 0.0).astype(jnp.float32)
    before = jnp.where(lax.broadcasted_iota(jnp.int32, (rows, rows), 0) > lax.broadcasted_iota(jnp.int32, (rows, rows), 1),
                       1.0, 0.0).astype(jnp.bfloat16)
    seen = jnp.dot(before, (hit0 + hit1).astype(jnp.bfloat16), preferred_element_type=jnp.float32)
    total0 = jnp.sum(hit0, axis=0, keepdims=True)
    pos0 = jnp.sum(seen * hit0, axis=1, keepdims=True)
    pos1 = jnp.sum(seen * hit1 + jnp.where(lane == ids1, total0, 0.0), axis=1, keepdims=True)

    def slot_of(ids, pos):
        block = ((((ids >> 1) - chip) & (CHIPS - 1)) << 1) | ((ids & 1) ^ core)
        return jnp.where(pos < cap, (block * cap).astype(jnp.float32) + pos, -1.0)

    slot0 = slot_of(ids0, pos0)
    slot1 = slot_of(ids1, pos1)
    slot_iota = lax.broadcasted_iota(jnp.int32, (rows, 384), 1).astype(jnp.float32)
    take0 = jnp.where(slot_iota == slot0, 1.0, 0.0)
    take1 = jnp.where(slot_iota == slot1, 1.0, 0.0)
    pick = jnp.transpose(take0 + take1)[:slots].astype(jnp.bfloat16)

    def dispatch(kc, wait_barrier):
        cols = pl.ds(k_off[kc], K_CHUNKS[kc])
        part = jnp.dot(pick, u_v[:, cols], preferred_element_type=jnp.float32).astype(jnp.bfloat16)
        stage[kc][pl.ds(0, slots), :] = part
        recv[kc][pl.ds(0, cap), :] = part[:cap]
        if wait_barrier:
            pl.semaphore_wait(barrier, BLOCKS - 1)
        for d, s in block_pairs():
            send_copy(kc, d, s).start()

    def send_copy(kc, d, s):
        b = d * 2 + s
        rb = ((CHIPS - d) % CHIPS) * 2 + s
        return pltpu.make_async_remote_copy(
            src_ref=stage[kc].at[pl.ds(b * cap, cap)], dst_ref=recv[kc].at[pl.ds(rb * cap, cap)],
            send_sem=ds_sem.at[kc], recv_sem=dr_sem.at[kc], device_id=peer(d, s))

    for kc in range(nk):
        with jax.named_scope(f'dispatch{kc}'):
            dispatch(kc, kc == 0)

    logits = lax.dot_general(u, router_v[...], (((1,), (1,)), ((), ())), preferred_element_type=jnp.float32)
    lane8 = lax.broadcasted_iota(jnp.int32, logits.shape, 1)
    pick0 = jnp.sum(jnp.where(lane8 == ids0, logits, 0.0), axis=1, keepdims=True)
    pick1 = jnp.sum(jnp.where(lane8 == ids1, logits, 0.0), axis=1, keepdims=True)
    top = jnp.maximum(pick0, pick1)
    e0 = jnp.exp(pick0 - top)
    e1 = jnp.exp(pick1 - top)
    gate0 = e0 / (e0 + e1)
    gate1 = e1 / (e0 + e1)
    fetch = jnp.concatenate([take0[:, :slots], take1[:, :slots]], axis=0).astype(jnp.bfloat16)

    for kc in range(nk):
        size = K_CHUNKS[kc]
        with jax.named_scope(f"recv{kc}"):
            wait_bytes(recv[kc].at[remote], dr_sem.at[kc])
        u2_v[:, pl.ds(0, size)] = recv[kc][pl.ds(0, slots), :]

        @pl.loop(0, n_f)
        def _(f):
            slot = (kc % 2) * n_f + f
            with jax.named_scope(f"weights{kc}"):
                wait_bytes(w_ring.at[slot, pl.ds(0, size)], w_sem.at[slot])
            prod = jnp.dot(u2_v[:, pl.ds(0, size)], w_ring[slot, pl.ds(0, size)], preferred_element_type=jnp.float32)
            if kc == 0:
                acc[f] = prod
            elif kc < nk - 1:
                acc[f] = acc[f] + prod
            else:
                g = acc[f, :, pl.ds(0, FCOLS)] + prod[:, :FCOLS]
                v = acc[f, :, pl.ds(FCOLS, FCOLS)] + prod[:, FCOLS:]
                h_v[:, pl.ds(pl.multiple_of(f * FCOLS, 128), FCOLS)] = (jax.nn.silu(g) * v).astype(jnp.bfloat16)
            if kc + 2 < nk:
                for cp in w_copies(kc + 2, f):
                    cp.start()

        if kc == nk - 3:
            for n in range(WD_SLOTS):
                wd_copy(n, n).start()

    def back_copy(n, r, s):
        b = r * 2 + s
        rb = ((CHIPS - r) % CHIPS) * 2 + s
        return pltpu.make_async_remote_copy(
            src_ref=o_stage.at[n, pl.ds(b * cap, cap)], dst_ref=back.at[n, pl.ds(rb * cap, cap)],
            send_sem=os_sem.at[n], recv_sem=or_sem.at[n], device_id=peer(r, s))

    @pl.loop(0, n_n)
    def _(n):
        slot = lax.rem(n, WD_SLOTS)
        with jax.named_scope('wd'):
            wd_copy(n, slot).wait()
        o = jnp.dot(h_v[...], wd_ring[slot], preferred_element_type=jnp.float32).astype(jnp.bfloat16)
        o_stage[n, pl.ds(0, slots)] = o
        back[n, pl.ds(0, cap)] = o[:cap]
        for r, s in block_pairs():
            back_copy(n, r, s).start()

        @pl.when(n + WD_SLOTS < n_n)
        def _():
            wd_copy(n + WD_SLOTS, slot).start()

    @pl.loop(0, n_n)
    def _(n):
        with jax.named_scope("back_recv"):
            wait_bytes(back.at[n, remote], or_sem.at[n])
        got = jnp.dot(fetch, back[n, pl.ds(0, slots)], preferred_element_type=jnp.float32)
        cols = pl.ds(pl.multiple_of(n * NCOLS, 128), NCOLS)
        y = gate0 * got[:rows] + gate1 * got[rows:]
        out_ref[:, cols] = (x_v[:, cols].astype(jnp.float32) + y).astype(jnp.bfloat16)

    for kc in range(nk):
        wait_bytes(stage[kc].at[remote], ds_sem.at[kc])

    @pl.loop(0, n_n)
    def _(n):
        wait_bytes(o_stage.at[n, remote], os_sem.at[n])


def solution(mesh):
    token_spec = P(("dp", "ep"), None)
    expert_spec = P("ep", None, None)

    def local_block(hidden, expert_ids, norm_gain, w_router, w_gate, w_up, w_down):
        rows, width = hidden.shape
        ff = w_gate.shape[2]
        experts = w_router.shape[1]
        cap = (5 * rows + 2 * experts - 1) // (2 * experts)
        slots = BLOCKS * cap
        padded = slots + 8
        n_f = ff // FCOLS
        n_n = width // NCOLS
        nk = len(K_CHUNKS)
        bf16, f32 = jnp.bfloat16, jnp.float32
        dma = pltpu.SemaphoreType.DMA
        hbm = pl.BlockSpec(memory_space=pl.ANY)
        return pl.pallas_call(
            functools.partial(moe_kernel, cap),
            out_shape=pltpu.VMEM((rows, width), bf16),
            in_specs=[hbm] * 7,
            out_specs=pl.BlockSpec(memory_space=pltpu.VMEM),
            scratch_shapes=[
                pltpu.VMEM((rows, width), bf16),
                pltpu.VMEM(expert_ids.shape[::-1], jnp.int32),
                pltpu.VMEM((width,), bf16),
                pltpu.VMEM(w_router.shape[::-1], bf16),
                pltpu.VMEM((rows, width), bf16),
                pltpu.VMEM((2 * n_f, max(K_CHUNKS), 2 * FCOLS), bf16),
                pltpu.VMEM((WD_SLOTS, ff, NCOLS), bf16),
                pltpu.VMEM((n_f, slots, 2 * FCOLS), f32),
                pltpu.VMEM((slots, ff), bf16),
                pltpu.VMEM((slots, max(K_CHUNKS)), bf16),
                pltpu.VMEM((n_n, padded, NCOLS), bf16),
                pltpu.VMEM((n_n, padded, NCOLS), bf16),
                *[pltpu.VMEM((padded, k), bf16) for k in K_CHUNKS],
                *[pltpu.VMEM((padded, k), bf16) for k in K_CHUNKS],
                dma((4,)),
                dma((2 * n_f,)),
                dma((WD_SLOTS,)),
                dma((nk,)),
                dma((nk,)),
                dma((n_n,)),
                dma((n_n,)),
            ],
            compiler_params=pltpu.CompilerParams(collective_id=0, has_side_effects=True, vmem_limit_bytes=64 * 1024 * 1000),
        )(hidden, expert_ids.T, norm_gain, w_router.T, w_gate, w_up, w_down)

    return jax.shard_map(local_block, mesh=mesh,
                         in_specs=(token_spec, token_spec, P(None), P(None, None), expert_spec, expert_spec, expert_spec),
                         out_specs=token_spec, check_vma=False)
```
